32 devices in a mesh: fsdp: 4 (over y, x), rep: 8 (over z, core).
Axes of the slice: x: 2, y: 2, z: 4, core: 2. Of those that a mesh axis runs over, the one named last changes fastest.
Arguments:
- inputs: bfloat16 [64, 128, 2048], P(('fsdp', 'rep')), may hold values from -6 to 6
- segment_ids: int32 [64, 128], P(('fsdp', 'rep')), may hold values from 0 to 3, never falling along the last dimension, each value on 1 to 64 neighbouring positions
- cotangent: bfloat16 [64, 128, 2048], P(('fsdp', 'rep')), may hold values from -6 to 6
- norm_gain: bfloat16 [2048], replicated, may hold values from 0.5 to 1.5
- norm_shift: bfloat16 [2048], replicated, may hold values from -4 to 4
- qkv_weight: bfloat16 [2048, 6144], P('fsdp'), may hold values from -0.125 to 0.125
- qkv_bias: bfloat16 [6144], replicated, may hold values from -6 to 6
- dense_weight: bfloat16 [2048, 2048], P('fsdp'), may hold values from -0.375 to 0.375
- dense_bias: bfloat16 [2048], replicated, may hold values from -4 to 4
- fc1_weight: bfloat16 [2048, 8192], P('fsdp'), may hold values from -0.125 to 0.125
- fc1_bias: bfloat16 [8192], replicated, may hold values from -6 to 6
- fc2_weight: bfloat16 [8192, 2048], P('fsdp'), may hold values from -0.125 to 0.125
- fc2_bias: bfloat16 [2048], replicated, may hold values from -4 to 4
Outputs:
- layer_output: bfloat16 [64, 128, 2048], P(('fsdp', 'rep'))
- input_grad: bfloat16 [64, 128, 2048], P(('fsdp', 'rep'))
- norm_gain_grad: float32 [2048], P('fsdp')
- norm_shift_grad: float32 [2048], P('fsdp')
- qkv_weight_grad: float32 [2048, 6144], P('fsdp')
- qkv_bias_grad: float32 [6144], P('fsdp')
- dense_weight_grad: float32 [2048, 2048], P('fsdp')
- dense_bias_grad: float32 [2048], P('fsdp')
- fc1_weight_grad: float32 [2048, 8192], P('fsdp')
- fc1_bias_grad: float32 [8192], P('fsdp')
- fc2_weight_grad: float32 [8192, 2048], P('fsdp')
- fc2_bias_grad: float32 [2048], P('fsdp')
The draws below stay inside these ranges and needn't reach their ends.
Inputs may be any that keep to these rules, and one draw needn't show every extreme that they name: `segment_ids`: along each sequence the document numbers never fall; every document has 1 to 64 tokens, and some document has exactly 64.
All inputs are finite; a program needn't handle non-finite values.
Results may differ from the reference program's by a relative error of at most 0.015.
Values may be sent and summed in bfloat16 or wider, within the bound.
A program may use at most 832 MiB of HBM per device.

```python
import math
import jax
import jax.numpy as jnp
import numpy as np
from jax import lax

D = 2048
HEADS = 32
HD = 64
ROT = 32
FF = 8192
SEQ = 128
SEQS = 64


def shard_levels(rng, dims, pieces, least, high):
    factor_of = 1.0
    for dim, blocks in pieces:
        heights = jax.random.uniform(jax.random.fold_in(jax.random.fold_in(rng, 6), dim), (blocks,), jnp.float32, least / len(pieces), high / len(pieces))
        factor_of = factor_of * jnp.repeat(jnp.exp(heights), dims[dim] // blocks).reshape((-1,) + (1,) * (len(dims) - 1 - dim))
    return factor_of


def split_up(count, total, reach, lean):
    portions = [(1 << 20) // math.isqrt(rank ** lean) + 1 for rank in range(2, count + 1)]
    rest, holding = total - reach - (count - 1), [1] * (count - 1)
    while rest > 0:
        movable = [i for i in range(count - 1) if holding[i] < reach]
        pool, remaining = sum([portions[i] for i in movable]), rest
        for i in movable:
            extra = min(reach - holding[i], max(1, remaining * portions[i] // pool), rest)
            holding[i] = holding[i] + extra
            rest = rest - extra
    return np.array([reach] + holding)


def uneven_parts(rng, number_of, total, most, skew):
    if number_of == 2:
        one = jax.random.randint(rng, (), max(1, total - most), min(most, total - 1) + 1)
        return jnp.stack([one, total - one])
    lengths = jnp.asarray(split_up(number_of, total, most, skew), jnp.int32)
    couples = (number_of - 1) // 2
    source_of, taker = lengths[1:1 + 2 * couples:2], lengths[2:2 + 2 * couples:2]
    room = jnp.minimum(source_of - 1, most - taker)
    moved = jax.random.randint(jax.random.fold_in(rng, 1), (couples,), 0, 1 << 20) % (room + 1)
    lengths = lengths.at[1:1 + 2 * couples:2].set(source_of - moved).at[2:2 + 2 * couples:2].set(taker + moved)
    return lengths[jax.random.permutation(jax.random.fold_in(rng, 2), number_of)]


def normal_values(key, dims, spread, reach, shards=(), kind=jnp.bfloat16):
    entries = spread * jax.random.normal(key, dims, jnp.float32)
    if shards:
        entries = entries * shard_levels(key, dims, shards, -0.22, 0.18)
    return jnp.clip(entries, -reach, reach).astype(kind)


def setup_inputs(seed: int = 0) -> dict:
    streams_of = jax.random.split(jax.random.key(seed), 14)
    return {
        "inputs": normal_values(streams_of[0], (SEQS, SEQ, D), 1.0, 6.0, ((0, 32),)),
        "segment_ids": jax.vmap(lambda own: jnp.searchsorted(jnp.cumsum(uneven_parts(own, 4, SEQ, SEQ // 2, 1)), jnp.arange(SEQ), side="right"))(jax.random.split(streams_of[1], SEQS)).reshape((SEQS, SEQ)).astype(jnp.int32),
        "cotangent": normal_values(streams_of[2], (SEQS, SEQ, D), 1.0, 6.0, ((0, 32),)),
        "norm_gain": jnp.clip(1.0 + 0.1 * jax.random.normal(streams_of[3], (D,), jnp.float32), 0.5, 1.5).astype(jnp.bfloat16),
        "norm_shift": normal_values(streams_of[4], (D,), 0.3, 4.0),
        "qkv_weight": normal_values(streams_of[5], (D, 3 * D), D ** -0.5, 0.125, ((0, 4),)),
        "qkv_bias": normal_values(streams_of[6], (3 * D,), 0.5, 6.0),
        "dense_weight": normal_values(streams_of[7], (D, D), (D // 8) ** -0.5, 0.375, ((0, 4),)),
        "dense_bias": normal_values(streams_of[8], (D,), 0.3, 4.0),
        "fc1_weight": normal_values(streams_of[9], (D, FF), D ** -0.5, 0.125, ((0, 4),)),
        "fc1_bias": normal_values(streams_of[10], (FF,), 0.5, 6.0),
        "fc2_weight": normal_values(streams_of[11], (FF, D), (FF // 4) ** -0.5, 0.125, ((0, 4),)),
        "fc2_bias": normal_values(streams_of[12], (D,), 0.3, 4.0),
    }


@jax.custom_vjp
def low(v):
    return lax.optimization_barrier(v.astype(jnp.bfloat16)).astype(jnp.float32)

@jax.custom_vjp
def low_back(v):
    return v

def low_keep(v):
    return (low(v), None)

def low_pass(kept, grad):
    return (grad,)

def back_keep(v):
    return (v, None)

def back_low(kept, grad):
    return (low(grad),)
low.defvjp(low_keep, low_pass)
low_back.defvjp(back_keep, back_low)
norm_eps = 1e-05
highest = lax.Precision.HIGHEST

def positions_of(segment_row):
    last_axis = segment_row.ndim - 1
    token_index = lax.broadcasted_iota(jnp.int32, segment_row.shape, last_axis)
    previous = jnp.concatenate([segment_row[..., :1] - 1, segment_row[..., :-1]], axis=last_axis)
    starts = jnp.where(segment_row != previous, token_index, 0)
    return token_index - lax.cummax(starts, axis=last_axis)

def rotary_tables(positions):
    half_rot = ROT // 2
    inv_freq = 10000.0 ** (-2.0 * jnp.arange(half_rot, dtype=jnp.float32) / ROT)
    angles = positions.astype(jnp.float32)[..., None] * inv_freq
    angles = jnp.concatenate([angles, angles], axis=-1)
    return (jnp.cos(angles), jnp.sin(angles))

def rotate(values, cos_tab, sine_tab):
    half_rot = ROT // 2
    turned = values[..., :ROT]
    swapped = jnp.concatenate([-turned[..., half_rot:], turned[..., :half_rot]], axis=-1)
    turned = turned * cos_tab[:, None, :] + swapped * sine_tab[:, None, :]
    return jnp.concatenate([turned, values[..., ROT:]], axis=-1)

def attend_seq(inputs_one):
    joined_seq, segment_row, cos_tab, sine_tab = inputs_one
    query_heads = low(rotate(joined_seq[:, 0], cos_tab, sine_tab))
    key_heads = low(rotate(joined_seq[:, 1], cos_tab, sine_tab))
    value_heads = low(joined_seq[:, 2])
    scores = low_back(jnp.einsum('qhd,khd->hqk', query_heads, key_heads, precision=highest) * HD ** (-0.5))
    token_index = jnp.arange(SEQ, dtype=jnp.int32)
    allowed = (token_index[:, None] >= token_index[None, :]) & (segment_row[:, None] == segment_row[None, :])
    scores = jnp.where(allowed[None], scores, -1e+30)
    attn_probs = low(jax.nn.softmax(scores, axis=-1))
    mixed_heads = jnp.einsum('hqk,khd->qhd', attn_probs, value_heads, precision=highest)
    return mixed_heads.reshape(SEQ, D)

def layer(params, block_in, segments):
    norm_gain, norm_shift, qkv_weight, qkv_bias, dense_weight, dense_bias, fc1_weight, fc1_bias, fc2_weight, fc2_bias = params
    seq_count = block_in.shape[0]
    token_rows = block_in.reshape(seq_count * SEQ, D)
    row_mean = lax.optimization_barrier(jnp.mean(token_rows, axis=-1, keepdims=True))
    centred = token_rows - row_mean
    row_var = lax.optimization_barrier(jnp.mean(centred * centred, axis=-1, keepdims=True))
    normed = low(centred * lax.rsqrt(row_var + norm_eps) * norm_gain + norm_shift)
    joined_qkv = low_back(jnp.dot(normed, qkv_weight, precision=highest, preferred_element_type=jnp.float32) + qkv_bias)
    pre_act = low_back(jnp.dot(normed, fc1_weight, precision=highest, preferred_element_type=jnp.float32) + fc1_bias)
    hidden = low(jax.nn.gelu(pre_act, approximate=True))
    mlp_out = jnp.dot(hidden, fc2_weight, precision=highest, preferred_element_type=jnp.float32) + fc2_bias
    cos_tab, sine_tab = rotary_tables(positions_of(segments))
    joined_seqs = joined_qkv.reshape(seq_count, SEQ, 3, HEADS, HD)
    mixed_rows = lax.map(jax.checkpoint(attend_seq), (joined_seqs, segments, cos_tab, sine_tab))
    mixed_rows = low(low_back(mixed_rows.reshape(seq_count * SEQ, D)))
    attn_out = jnp.dot(mixed_rows, dense_weight, precision=highest, preferred_element_type=jnp.float32) + dense_bias
    return (token_rows + attn_out + mlp_out).reshape(block_in.shape)

def reference(inputs, segment_ids, cotangent, norm_gain, norm_shift, qkv_weight, qkv_bias, dense_weight, dense_bias, fc1_weight, fc1_bias, fc2_weight, fc2_bias):
    params = tuple((param_in.astype(jnp.float32) for param_in in (norm_gain, norm_shift, qkv_weight, qkv_bias, dense_weight, dense_bias, fc1_weight, fc1_bias, fc2_weight, fc2_bias)))
    group_size = 16
    group_count = SEQS // group_size
    input_groups = inputs.reshape(group_count, group_size, SEQ, D)
    segment_groups = segment_ids.reshape(group_count, group_size, SEQ)
    back_groups = cotangent.reshape(group_count, group_size, SEQ, D)

    def one_group(running, group_in):
        block_in, segments, back_in = group_in

        def forward(param_set, values_in):
            return layer(param_set, values_in, segments)
        layer_out, pull_back = jax.vjp(forward, params, block_in.astype(jnp.float32))
        param_grads, input_part = pull_back(back_in.astype(jnp.float32))
        running = jax.tree.map(jnp.add, running, param_grads)
        return (running, (layer_out.astype(jnp.bfloat16), input_part.astype(jnp.bfloat16)))
    grad_zeros = jax.tree.map(jnp.zeros_like, params)
    totals, (layer_outs, input_grads) = lax.scan(one_group, grad_zeros, (input_groups, segment_groups, back_groups))
    return (layer_outs.reshape(SEQS, SEQ, D), input_grads.reshape(SEQS, SEQ, D), totals[0], totals[1], totals[2], totals[3], totals[4], totals[5], totals[6], totals[7], totals[8], totals[9])
```

```python
import jax
import jax.numpy as jnp
from jax import lax
from jax.sharding import PartitionSpec as P

HD = 64
ROT = 32
norm_eps = 1e-05
CHUNKS_A = 5
CHUNKS_B = 4


AXES = ("fsdp", "rep")


def positions_of(segment_row):
    last_axis = segment_row.ndim - 1
    token_index = lax.broadcasted_iota(jnp.int32, segment_row.shape, last_axis)
    previous = jnp.concatenate([segment_row[..., :1] - 1, segment_row[..., :-1]], axis=last_axis)
    starts = jnp.where(segment_row != previous, token_index, 0)
    return token_index - lax.cummax(starts, axis=last_axis)


def rotary_tables(positions):
    half_rot = ROT // 2
    inv_freq = 10000.0 ** (-2.0 * jnp.arange(half_rot, dtype=jnp.float32) / ROT)
    angles = positions.astype(jnp.float32)[..., None] * inv_freq
    angles = jnp.concatenate([angles, angles], axis=-1)
    return (jnp.cos(angles), jnp.sin(angles))


def rotate(values, cos_tab, sine_tab):
    half_rot = ROT // 2
    turned = values[..., :ROT]
    swapped = jnp.concatenate([-turned[..., half_rot:], turned[..., :half_rot]], axis=-1)
    turned = turned * cos_tab[..., None, :] + swapped * sine_tab[..., None, :]
    return jnp.concatenate([turned, values[..., ROT:]], axis=-1)


def rotate_back(grad_in, cos_tab, sine_tab):
    half_rot = ROT // 2
    rot_part = grad_in[..., :ROT]
    scaled = rot_part * sine_tab[..., None, :]
    rot_back = jnp.concatenate([scaled[..., half_rot:], -scaled[..., :half_rot]], axis=-1)
    rot_part = rot_part * cos_tab[..., None, :] + rot_back
    return jnp.concatenate([rot_part, grad_in[..., ROT:]], axis=-1)


def dot_plain(left_op, right_op):
    return jnp.dot(left_op, right_op, preferred_element_type=jnp.float32)


def dot_last(left_op, right_op):
    return lax.dot_general(
        left_op, right_op, (((1,), (1,)), ((), ())), preferred_element_type=jnp.float32
    )


def dot_first(left_op, right_op):
    return lax.dot_general(
        left_op, right_op, (((0,), (0,)), ((), ())), preferred_element_type=jnp.float32
    )


def gelu_parts(pre_act):
    scale = 0.7978845608028654
    cubic = 0.044715
    squared = pre_act * pre_act
    tanh_val = jnp.tanh(scale * (pre_act + cubic * squared * pre_act))
    value = 0.5 * pre_act * (1.0 + tanh_val)
    slope = 0.5 * (1.0 + tanh_val) + 0.5 * pre_act * (1.0 - tanh_val * tanh_val) * scale * (
        1.0 + 3.0 * cubic * squared
    )
    return value, slope


def make_per_device(groups, reps):
    places = reps // 2

    def send_to(target):
        pairs = []
        for group in range(groups):
            for rep in range(reps):
                to = target(group, rep)
                if to is not None:
                    pairs.append((group * reps + rep, to[0] * reps + to[1]))
        return pairs

    to_core = send_to(lambda g, r: (g, r ^ 1))
    to_right = send_to(lambda g, r: (g, r + 2) if r + 2 < reps else None)
    to_left = send_to(lambda g, r: (g, r - 2) if r >= 2 else None)

    def move(value, pairs):
        return lax.ppermute(value, AXES, pairs)

    def swap(value):
        return move(value, to_core)

    def exchange(blocks_of, group):
        own = blocks_of(group)
        out = jnp.zeros((groups,) + own.shape, own.dtype)
        out = lax.dynamic_update_index_in_dim(out, own, group, 0)
        for offset in range(1, groups):
            got = move(blocks_of(group ^ offset), send_to(lambda g, r: (g ^ offset, r)))
            out = lax.dynamic_update_index_in_dim(out, got, group ^ offset, 0)
        return out

    def total_of(vector):
        step = 1
        while step < groups:
            vector = vector + move(vector, send_to(lambda g, r: (g ^ step, r)))
            step *= 2
        step = 1
        while step < reps:
            vector = vector + move(vector, send_to(lambda g, r: (g, r ^ step)))
            step *= 2
        return vector

    def line_sum(own, chunks, place):
        rows = own.shape[0] // chunks
        parts = own.reshape((chunks, rows) + own.shape[1:])
        steps = chunks + places - 2
        from_left, from_right = [], []
        held_left = held_right = None
        for step in range(steps):
            right_out = lax.dynamic_index_in_dim(
                parts, jnp.clip(step - place, 0, chunks - 1), 0, keepdims=False
            )
            left_out = lax.dynamic_index_in_dim(
                parts, jnp.clip(step - (places - 1 - place), 0, chunks - 1), 0, keepdims=False
            )
            if held_left is not None:
                right_out = (right_out.astype(jnp.float32) + held_left.astype(jnp.float32)).astype(
                    jnp.bfloat16
                )
                left_out = (left_out.astype(jnp.float32) + held_right.astype(jnp.float32)).astype(
                    jnp.bfloat16
                )
            held_left = move(right_out, to_right)
            held_right = move(left_out, to_left)
            from_left.append(held_left)
            from_right.append(held_right)
        blank = jnp.zeros_like(from_left[0])
        left_all = jnp.stack([blank] + from_left)
        right_all = jnp.stack([blank] + from_right)
        prefix = lax.dynamic_slice_in_dim(left_all, place, chunks, 0)
        suffix = lax.dynamic_slice_in_dim(right_all, places - 1 - place, chunks, 0)
        has_left = (place > 0).astype(jnp.float32)
        has_right = (place < places - 1).astype(jnp.float32)
        total = (
            parts.astype(jnp.float32)
            + prefix.astype(jnp.float32) * has_left
            + suffix.astype(jnp.float32) * has_right
        )
        return total.astype(jnp.bfloat16).reshape(own.shape)

    def per_device(
        inputs,
        segment_ids,
        cotangent,
        norm_gain,
        norm_shift,
        qkv_weight,
        qkv_bias,
        dense_weight,
        dense_bias,
        fc1_weight,
        fc1_bias,
        fc2_weight,
        fc2_bias,
    ):
        seqs, seq_len, width = inputs.shape
        tokens = seqs * seq_len
        ffn = fc1_weight.shape[1]
        head_cols = width // groups // 2
        ffn_cols = ffn // groups // 2
        half_heads = width // HD // 2
        score_scale = HD ** (-0.5)
        group = lax.axis_index("fsdp")
        rep = lax.axis_index("rep")
        core = rep % 2
        place = rep // 2

        def halves(array, cut_axis):
            mine = lax.dynamic_index_in_dim(array, core, cut_axis, keepdims=False)
            other = lax.dynamic_index_in_dim(array, 1 - core, cut_axis, keepdims=False)
            return mine, other

        def ordered(mine, other, axis):
            first = jnp.where(core == 0, mine, other)
            second = jnp.where(core == 0, other, mine)
            return jnp.stack([first, second], axis=axis)

        def gathered(mine):
            return lax.all_gather(mine, "fsdp", axis=0, tiled=True)

        rows = qkv_weight.shape[0]
        qkv_view = qkv_weight.reshape(rows, 3, groups, 2, head_cols)
        qkv_own = lax.dynamic_index_in_dim(qkv_view, core, 3, keepdims=False).reshape(rows, -1)
        fc1_view = fc1_weight.reshape(rows, groups, 2, ffn_cols)
        fc1_own = lax.dynamic_index_in_dim(fc1_view, core, 2, keepdims=False).reshape(rows, -1)
        dense_own = lax.dynamic_slice_in_dim(dense_weight, core * head_cols, head_cols, 0)
        fc2_own = lax.dynamic_slice_in_dim(fc2_weight, core * ffn_cols, ffn_cols, 0)
        qkv_mine = gathered(qkv_own)
        qkv_other = swap(qkv_mine)
        dense_mine = gathered(dense_own)
        dense_other = swap(dense_mine)
        back_b = cotangent.reshape(tokens, width)
        back_mine = gathered(back_b)
        back_other = swap(back_mine)
        fc1_mine = gathered(fc1_own)
        fc1_other = swap(fc1_mine)
        fc2_mine = gathered(fc2_own)
        fc2_other = swap(fc2_mine)

        gain_f32 = norm_gain.astype(jnp.float32)
        shift_f32 = norm_shift.astype(jnp.float32)
        qkv_bias_mine, qkv_bias_other = halves(
            qkv_bias.astype(jnp.float32).reshape(3, groups, 2, head_cols), 2
        )
        fc1_bias_mine, fc1_bias_other = halves(
            fc1_bias.astype(jnp.float32).reshape(groups, 2, ffn_cols), 1
        )
        token_rows = inputs.reshape(tokens, width).astype(jnp.float32)
        row_mean = jnp.mean(token_rows, axis=-1, keepdims=True)
        centred = token_rows - row_mean
        row_var = jnp.mean(centred * centred, axis=-1, keepdims=True)
        inv_std = lax.rsqrt(row_var + norm_eps)
        x_hat = centred * inv_std
        normed = (x_hat * gain_f32 + shift_f32).astype(jnp.bfloat16)

        normed_cut = normed.reshape(tokens, groups, rows)
        normed_mine = exchange(
            lambda k: lax.dynamic_index_in_dim(normed_cut, k, 1, keepdims=False), group
        )
        normed_other = swap(normed_mine)
        normed_all = jnp.stack([normed_mine, normed_other], axis=1).reshape(-1, rows)

        cos_tab, sine_tab = rotary_tables(positions_of(segment_ids))
        index = jnp.arange(seq_len, dtype=jnp.int32)
        allowed = (index[:, None] >= index[None, :])[None] & (
            segment_ids[:, :, None] == segment_ids[:, None, :]
        )

        def attend(weight, bias):
            joined = dot_plain(normed, weight) + bias.reshape(-1)
            heads = joined.reshape(seqs, seq_len, 3, half_heads, HD)
            query_b = rotate(heads[:, :, 0], cos_tab, sine_tab).astype(jnp.bfloat16)
            key_b = rotate(heads[:, :, 1], cos_tab, sine_tab).astype(jnp.bfloat16)
            value_b = heads[:, :, 2].astype(jnp.bfloat16)
            scores = (
                jnp.einsum("bqhd,bkhd->bhqk", query_b, key_b, preferred_element_type=jnp.float32)
                * score_scale
            )
            scores = jnp.where(allowed[:, None], scores, -1e30)
            row_max = jnp.max(scores, axis=-1, keepdims=True)
            exp_scores = jnp.exp(scores - row_max)
            probs = exp_scores / jnp.sum(exp_scores, axis=-1, keepdims=True)
            mixed = jnp.einsum(
                "bhqk,bkhd->bqhd",
                probs.astype(jnp.bfloat16),
                value_b,
                preferred_element_type=jnp.float32,
            )
            return query_b, key_b, value_b, probs, mixed.reshape(tokens, -1).astype(jnp.bfloat16)

        def attend_back(kept, weight):
            query_b, key_b, value_b, probs, _ = kept
            d_mixed = dot_last(back_b, weight).astype(jnp.bfloat16)
            d_mixed = d_mixed.reshape(seqs, seq_len, half_heads, HD)
            d_probs = jnp.einsum(
                "bqhd,bkhd->bhqk", d_mixed, value_b, preferred_element_type=jnp.float32
            )
            d_value = jnp.einsum(
                "bhqk,bqhd->bkhd",
                probs.astype(jnp.bfloat16),
                d_mixed,
                preferred_element_type=jnp.float32,
            )
            d_scores = (
                probs * (d_probs - jnp.sum(probs * d_probs, axis=-1, keepdims=True))
            ).astype(jnp.bfloat16)
            d_query = (
                jnp.einsum("bhqk,bkhd->bqhd", d_scores, key_b, preferred_element_type=jnp.float32)
                * score_scale
            )
            d_key = (
                jnp.einsum("bhqk,bqhd->bkhd", d_scores, query_b, preferred_element_type=jnp.float32)
                * score_scale
            )
            d_query = rotate_back(d_query, cos_tab, sine_tab)
            d_key = rotate_back(d_key, cos_tab, sine_tab)
            return jnp.concatenate(
                [
                    part.reshape(tokens, half_heads * HD).astype(jnp.bfloat16)
                    for part in (d_query, d_key, d_value)
                ],
                axis=1,
            )

        kept_mine = attend(qkv_mine, qkv_bias_mine)
        kept_other = attend(qkv_other, qkv_bias_other)
        d_joined_mine = attend_back(kept_mine, dense_mine)
        d_joined_other = attend_back(kept_other, dense_other)
        joined_pair = jnp.stack([d_joined_mine, swap(d_joined_other)])
        joined_all = gathered(joined_pair).reshape(-1, d_joined_mine.shape[1])

        def feed(weight, bias):
            pre_act = dot_plain(normed, weight) + bias.reshape(-1)
            value, slope = gelu_parts(pre_act)
            return value.astype(jnp.bfloat16), slope

        hidden_mine, slope_mine = feed(fc1_mine, fc1_bias_mine)
        hidden_other, slope_other = feed(fc1_other, fc1_bias_other)
        d_pre_mine = (dot_last(back_b, fc2_mine) * slope_mine).astype(jnp.bfloat16)
        d_pre_other = (dot_last(back_b, fc2_other) * slope_other).astype(jnp.bfloat16)
        pre_pair = jnp.stack([d_pre_mine, swap(d_pre_other)])
        pre_all = gathered(pre_pair).reshape(-1, d_pre_mine.shape[1])

        out_sum = dot_plain(kept_mine[4], dense_mine) + dot_plain(kept_other[4], dense_other)
        out_sum = out_sum + dot_plain(hidden_mine, fc2_mine) + dot_plain(hidden_other, fc2_other)
        layer_out = (
            token_rows
            + out_sum
            + dense_bias.astype(jnp.float32)
            + fc2_bias.astype(jnp.float32)
        ).astype(jnp.bfloat16)

        def act_cut(mixed, hidden):
            return jnp.concatenate(
                [
                    mixed.reshape(tokens, groups, head_cols),
                    hidden.reshape(tokens, groups, ffn_cols),
                ],
                axis=2,
            )

        acts = jnp.stack(
            [act_cut(kept_mine[4], hidden_mine), swap(act_cut(kept_other[4], hidden_other))]
        )
        acts_all = exchange(
            lambda k: lax.dynamic_index_in_dim(acts, k, 2, keepdims=False), group
        ).reshape(-1, head_cols + ffn_cols)
        back_all = jnp.stack(
            [
                back_mine.reshape(groups, tokens, width),
                back_other.reshape(groups, tokens, width),
            ],
            axis=1,
        ).reshape(-1, width)

        second_own = dot_first(acts_all, back_all).astype(jnp.bfloat16)
        second_mine = line_sum(second_own, CHUNKS_A, place)
        second_other = swap(second_mine)
        qkv_grad_own = dot_first(normed_all, joined_all).astype(jnp.bfloat16)
        qkv_grad_mine = line_sum(qkv_grad_own, CHUNKS_B, place)
        qkv_grad_other = swap(qkv_grad_mine)
        fc1_grad_own = dot_first(normed_all, pre_all).astype(jnp.bfloat16)
        fc1_grad_mine = line_sum(fc1_grad_own, CHUNKS_B, place)
        fc1_grad_other = swap(fc1_grad_mine)

        d_normed = (
            dot_last(d_joined_mine, qkv_mine)
            + dot_last(d_joined_other, qkv_other)
            + dot_last(d_pre_mine, fc1_mine)
            + dot_last(d_pre_other, fc1_other)
        )
        gain_sum = jnp.sum(d_normed * x_hat, axis=0)
        shift_sum = jnp.sum(d_normed, axis=0)
        d_hat = d_normed * gain_f32
        d_input = inv_std * (
            d_hat
            - jnp.mean(d_hat, axis=-1, keepdims=True)
            - x_hat * jnp.mean(d_hat * x_hat, axis=-1, keepdims=True)
        )
        back_f32 = back_b.astype(jnp.float32)
        input_grad = (back_f32 + d_input).astype(jnp.bfloat16)

        def column_sum(value):
            return jnp.sum(value, axis=0, dtype=jnp.float32)

        qkv_bias_sum = ordered(
            column_sum(d_joined_mine).reshape(3, groups, head_cols),
            column_sum(d_joined_other).reshape(3, groups, head_cols),
            2,
        ).reshape(-1)
        fc1_bias_sum = ordered(
            column_sum(d_pre_mine).reshape(groups, ffn_cols),
            column_sum(d_pre_other).reshape(groups, ffn_cols),
            1,
        ).reshape(-1)
        small = [gain_sum, shift_sum, qkv_bias_sum, column_sum(back_f32), fc1_bias_sum]
        small_total = total_of(jnp.concatenate(small))
        owned, start = [], 0
        for piece in small:
            count = piece.shape[0] // groups
            owned.append(lax.dynamic_slice_in_dim(small_total, start + group * count, count, 0))
            start += piece.shape[0]

        qkv_grad = ordered(
            qkv_grad_mine.reshape(rows, 3, groups, head_cols),
            qkv_grad_other.reshape(rows, 3, groups, head_cols),
            3,
        ).reshape(rows, -1)
        fc1_grad = ordered(
            fc1_grad_mine.reshape(rows, groups, ffn_cols),
            fc1_grad_other.reshape(rows, groups, ffn_cols),
            2,
        ).reshape(rows, -1)
        dense_grad = ordered(second_mine[:head_cols], second_other[:head_cols], 0)
        fc2_grad = ordered(second_mine[head_cols:], second_other[head_cols:], 0)
        return (
            layer_out.reshape(inputs.shape),
            input_grad.reshape(inputs.shape),
            owned[0],
            owned[1],
            qkv_grad.astype(jnp.float32),
            owned[2],
            dense_grad.reshape(-1, width).astype(jnp.float32),
            owned[3],
            fc1_grad.astype(jnp.float32),
            owned[4],
            fc2_grad.reshape(-1, width).astype(jnp.float32),
            owned[3],
        )

    return per_device


def solution(mesh):
    placed = (
        P(AXES, None, None),
        P(AXES, None),
        P(AXES, None, None),
        P(),
        P(),
        P("fsdp", None),
        P(),
        P("fsdp", None),
        P(),
        P("fsdp", None),
        P(),
        P("fsdp", None),
        P(),
    )
    return jax.shard_map(
        make_per_device(mesh.shape["fsdp"], mesh.shape["rep"]),
        mesh=mesh,
        in_specs=placed,
        out_specs=(
            P(AXES, None, None),
            P(AXES, None, None),
            P("fsdp"),
            P("fsdp"),
            P("fsdp", None),
            P("fsdp"),
            P("fsdp", None),
            P("fsdp"),
            P("fsdp", None),
            P("fsdp"),
            P("fsdp", None),
            P("fsdp"),
        ),
        check_vma=False,
    )
```

```python
import jax
import jax.numpy as jnp
from jax import lax
from jax.experimental import pallas as pl
from jax.experimental.pallas import tpu as pltpu
from jax.sharding import PartitionSpec as P

HD = 64
ROT = 32
norm_eps = 1e-05
CHUNKS_A = 5
CHUNKS_B = 4
CHUNKS_C = 4
PRE_PIECES = 2


AXES = ("fsdp", "rep")


def positions_of(segment_row):
    last_axis = segment_row.ndim - 1
    token_index = lax.broadcasted_iota(jnp.int32, segment_row.shape, last_axis)
    previous = jnp.concatenate([segment_row[..., :1] - 1, segment_row[..., :-1]], axis=last_axis)
    starts = jnp.where(segment_row != previous, token_index, 0)
    return token_index - lax.cummax(starts, axis=last_axis)


def rotary_tables(positions):
    half_rot = ROT // 2
    inv_freq = 10000.0 ** (-2.0 * jnp.arange(half_rot, dtype=jnp.float32) / ROT)
    angles = positions.astype(jnp.float32)[..., None] * inv_freq
    angles = jnp.concatenate([angles, angles], axis=-1)
    return (jnp.cos(angles), jnp.sin(angles))


def rotate(values, cos_tab, sine_tab):
    half_rot = ROT // 2
    turned = values[..., :ROT]
    swapped = jnp.concatenate([-turned[..., half_rot:], turned[..., :half_rot]], axis=-1)
    turned = turned * cos_tab[..., None, :] + swapped * sine_tab[..., None, :]
    return jnp.concatenate([turned, values[..., ROT:]], axis=-1)


def rotate_back(grad_in, cos_tab, sine_tab):
    half_rot = ROT // 2
    rot_part = grad_in[..., :ROT]
    scaled = rot_part * sine_tab[..., None, :]
    rot_back = jnp.concatenate([scaled[..., half_rot:], -scaled[..., :half_rot]], axis=-1)
    rot_part = rot_part * cos_tab[..., None, :] + rot_back
    return jnp.concatenate([rot_part, grad_in[..., ROT:]], axis=-1)


def dot_plain(left_op, right_op):
    return jnp.dot(left_op, right_op, preferred_element_type=jnp.float32)


def dot_last(left_op, right_op):
    return lax.dot_general(
        left_op, right_op, (((1,), (1,)), ((), ())), preferred_element_type=jnp.float32
    )


def dot_first(left_op, right_op):
    return lax.dot_general(
        left_op, right_op, (((0,), (0,)), ((), ())), preferred_element_type=jnp.float32
    )


def gelu_parts(pre_act):
    scale = 0.7978845608028654
    cubic = 0.044715
    squared = pre_act * pre_act
    tanh_val = jnp.tanh(scale * (pre_act + cubic * squared * pre_act))
    value = 0.5 * pre_act * (1.0 + tanh_val)
    slope = 0.5 * (1.0 + tanh_val) + 0.5 * pre_act * (1.0 - tanh_val * tanh_val) * scale * (
        1.0 + 3.0 * cubic * squared
    )
    return value, slope


def assemble(core_index, mine_parts, other_parts, first_row, rows):
    count = len(mine_parts)
    cols = mine_parts[0].shape[1]
    step = 64

    def kernel(core_ref, *refs):
        out_ref = refs[-1]
        is_mine = pl.program_id(1) == core_ref[0]

        for k in range(count):

            @pl.when(is_mine)
            def _():
                out_ref[:, k * cols : (k + 1) * cols] = refs[k][...].astype(jnp.float32)

            @pl.when(jnp.logical_not(is_mine))
            def _():
                out_ref[:, k * cols : (k + 1) * cols] = refs[count + k][...].astype(jnp.float32)

    block = pl.BlockSpec((step, cols), lambda i, h, c: (i + first_row // step, 0))
    return pl.pallas_call(
        kernel,
        out_shape=jax.ShapeDtypeStruct((rows, 2 * count * cols), jnp.float32),
        grid_spec=pltpu.PrefetchScalarGridSpec(
            num_scalar_prefetch=1,
            grid=(rows // step, 2),
            in_specs=[block] * (2 * count),
            out_specs=pl.BlockSpec((step, count * cols), lambda i, h, c: (i, h)),
        ),
        cost_estimate=pl.CostEstimate(
            flops=0, transcendentals=0, bytes_accessed=rows * count * cols * 12
        ),
    )(core_index, *mine_parts, *other_parts)


def make_per_device(groups, reps):
    places = reps // 2

    def send_to(target):
        pairs = []
        for group in range(groups):
            for rep in range(reps):
                to = target(group, rep)
                if to is not None:
                    pairs.append((group * reps + rep, to[0] * reps + to[1]))
        return pairs

    to_core = send_to(lambda g, r: (g, r ^ 1))
    to_right = send_to(lambda g, r: (g, r + 2) if r + 2 < reps else None)
    to_left = send_to(lambda g, r: (g, r - 2) if r >= 2 else None)

    def move(value, pairs):
        return lax.ppermute(value, AXES, pairs)

    def swap(value):
        return move(value, to_core)

    def exchange(blocks_of, group):
        own = blocks_of(group)
        out = jnp.zeros((groups,) + own.shape, own.dtype)
        out = lax.dynamic_update_index_in_dim(out, own, group, 0)
        for offset in range(1, groups):
            got = move(blocks_of(group ^ offset), send_to(lambda g, r: (g ^ offset, r)))
            out = lax.dynamic_update_index_in_dim(out, got, group ^ offset, 0)
        return out

    def total_of(vector):
        step = 1
        while step < groups:
            vector = vector + move(vector, send_to(lambda g, r: (g ^ step, r)))
            step *= 2
        step = 1
        while step < reps:
            vector = vector + move(vector, send_to(lambda g, r: (g, r ^ step)))
            step *= 2
        return vector

    def line_sum(own, chunks, place):
        rows = own.shape[0] // chunks
        parts = own.reshape((chunks, rows) + own.shape[1:])
        steps = chunks + places - 2
        from_left, from_right = [], []
        held_left = held_right = None
        for step in range(steps):
            right_out = lax.dynamic_index_in_dim(
                parts, jnp.clip(step - place, 0, chunks - 1), 0, keepdims=False
            )
            left_out = lax.dynamic_index_in_dim(
                parts, jnp.clip(step - (places - 1 - place), 0, chunks - 1), 0, keepdims=False
            )
            if held_left is not None:
                right_out = (right_out.astype(jnp.float32) + held_left.astype(jnp.float32)).astype(
                    jnp.bfloat16
                )
                left_out = (left_out.astype(jnp.float32) + held_right.astype(jnp.float32)).astype(
                    jnp.bfloat16
                )
            held_left = move(right_out, to_right)
            held_right = move(left_out, to_left)
            from_left.append(held_left)
            from_right.append(held_right)
        blank = jnp.zeros_like(from_left[0])
        left_all = jnp.stack([blank] + from_left)
        right_all = jnp.stack([blank] + from_right)
        prefix = lax.dynamic_slice_in_dim(left_all, place, chunks, 0)
        suffix = lax.dynamic_slice_in_dim(right_all, places - 1 - place, chunks, 0)
        has_left = (place > 0).astype(jnp.float32)
        has_right = (place < places - 1).astype(jnp.float32)
        total = (
            parts.astype(jnp.float32)
            + prefix.astype(jnp.float32) * has_left
            + suffix.astype(jnp.float32) * has_right
        )
        return total.astype(jnp.bfloat16).reshape(own.shape)

    def per_device(
        inputs,
        segment_ids,
        cotangent,
        norm_gain,
        norm_shift,
        qkv_weight,
        qkv_bias,
        dense_weight,
        dense_bias,
        fc1_weight,
        fc1_bias,
        fc2_weight,
        fc2_bias,
    ):
        seqs, seq_len, width = inputs.shape
        tokens = seqs * seq_len
        rows = qkv_weight.shape[0]
        half_rows = rows // 2
        fc2_rows = fc2_weight.shape[0]
        heads_all = width // HD
        score_scale = HD ** (-0.5)
        group = lax.axis_index("fsdp")
        rep = lax.axis_index("rep")
        core = rep % 2
        place = rep // 2

        def cut(array, index, axis):
            size = array.shape[axis] // 2
            return lax.dynamic_slice_in_dim(array, index * size, size, axis)

        def joined_halves(mine, other):
            first = jnp.where(core == 0, mine, other)
            second = jnp.where(core == 0, other, mine)
            return jnp.concatenate([first, second], axis=1)

        def row_cols(array):
            parts = [
                array[:, k * half_rows : (k + 1) * half_rows] for k in range(2 * groups)
            ]
            low, high = parts[0::2], parts[1::2]
            mine = [jnp.where(core == 0, x, y) for x, y in zip(low, high)]
            other = [jnp.where(core == 0, y, x) for x, y in zip(low, high)]
            return jnp.concatenate(mine, axis=1), jnp.concatenate(other, axis=1)

        def row_cols_back(mine, other):
            out = []
            for k in range(groups):
                x = mine[:, k * half_rows : (k + 1) * half_rows]
                y = other[:, k * half_rows : (k + 1) * half_rows]
                out.append(jnp.where(core == 0, x, y))
                out.append(jnp.where(core == 0, y, x))
            return jnp.concatenate(out, axis=1)

        def gathered(mine):
            return lax.all_gather(mine, "fsdp", axis=0, tiled=True)

        def plane_cols(value):
            pair = jnp.stack([cut(value, core, 1), swap(cut(value, 1 - core, 1))])
            return gathered(pair).reshape(-1, value.shape[1] // 2)

        qkv_mine = gathered(cut(qkv_weight, core, 0))
        qkv_other = swap(qkv_mine)
        dense_mine = gathered(cut(dense_weight, core, 1))
        dense_other = swap(dense_mine)
        back_b = cotangent.reshape(tokens, width)
        back_all = plane_cols(back_b)
        fc1_mine = gathered(cut(fc1_weight, core, 0))
        fc2_mine = gathered(cut(fc2_weight, core, 1))

        gain_f32 = norm_gain.astype(jnp.float32)
        shift_f32 = norm_shift.astype(jnp.float32)
        token_rows = inputs.reshape(tokens, width).astype(jnp.float32)
        row_mean = jnp.mean(token_rows, axis=-1, keepdims=True)
        centred = token_rows - row_mean
        row_var = jnp.mean(centred * centred, axis=-1, keepdims=True)
        inv_std = lax.rsqrt(row_var + norm_eps)
        x_hat = centred * inv_std
        normed = (x_hat * gain_f32 + shift_f32).astype(jnp.bfloat16)
        normed_in_mine, normed_in_other = row_cols(normed)
        back_cut_mine = cut(back_b, core, 1)
        back_cut_other = cut(back_b, 1 - core, 1)

        def plane_rows(blocks_of):
            own = exchange(blocks_of, group)
            return jnp.stack([own, swap(own)], axis=1).reshape(-1, own.shape[-1])

        normed_all = plane_rows(lambda k: lax.dynamic_slice_in_dim(normed, k * rows, rows, 1))

        cos_tab, sine_tab = rotary_tables(positions_of(segment_ids))
        index = jnp.arange(seq_len, dtype=jnp.int32)
        allowed = (index[:, None] >= index[None, :])[None] & (
            segment_ids[:, :, None] == segment_ids[:, None, :]
        )

        joined = dot_plain(normed_in_mine, qkv_mine) + dot_plain(normed_in_other, qkv_other)
        joined = joined + qkv_bias.astype(jnp.float32)
        heads = joined.reshape(seqs, seq_len, 3, heads_all, HD)
        query_b = rotate(heads[:, :, 0], cos_tab, sine_tab).astype(jnp.bfloat16)
        key_b = rotate(heads[:, :, 1], cos_tab, sine_tab).astype(jnp.bfloat16)
        value_b = heads[:, :, 2].astype(jnp.bfloat16)
        scores = (
            jnp.einsum("bqhd,bkhd->bhqk", query_b, key_b, preferred_element_type=jnp.float32)
            * score_scale
        )
        scores = jnp.where(allowed[:, None], scores, -1e30)
        row_max = jnp.max(scores, axis=-1, keepdims=True)
        exp_scores = jnp.exp(scores - row_max)
        probs = exp_scores / jnp.sum(exp_scores, axis=-1, keepdims=True)
        probs_b = probs.astype(jnp.bfloat16)
        mixed = jnp.einsum("bhqk,bkhd->bqhd", probs_b, value_b, preferred_element_type=jnp.float32)
        mixed_b = mixed.reshape(tokens, width).astype(jnp.bfloat16)

        d_mixed = dot_last(back_cut_mine, dense_mine) + dot_last(back_cut_other, dense_other)
        d_mixed = d_mixed.astype(jnp.bfloat16).reshape(seqs, seq_len, heads_all, HD)
        d_probs = jnp.einsum("bqhd,bkhd->bhqk", d_mixed, value_b, preferred_element_type=jnp.float32)
        d_value = jnp.einsum("bhqk,bqhd->bkhd", probs_b, d_mixed, preferred_element_type=jnp.float32)
        d_scores = (
            probs * (d_probs - jnp.sum(probs * d_probs, axis=-1, keepdims=True))
        ).astype(jnp.bfloat16)
        d_query = (
            jnp.einsum("bhqk,bkhd->bqhd", d_scores, key_b, preferred_element_type=jnp.float32)
            * score_scale
        )
        d_key = (
            jnp.einsum("bhqk,bqhd->bkhd", d_scores, query_b, preferred_element_type=jnp.float32)
            * score_scale
        )
        d_query = rotate_back(d_query, cos_tab, sine_tab)
        d_key = rotate_back(d_key, cos_tab, sine_tab)
        d_joined = jnp.concatenate(
            [part.reshape(tokens, width).astype(jnp.bfloat16) for part in (d_query, d_key, d_value)],
            axis=1,
        )

        fc1_mine, d_joined = lax.optimization_barrier((fc1_mine, d_joined))
        fc1_other = swap(fc1_mine)
        pre_act = dot_plain(normed_in_mine, fc1_mine) + dot_plain(normed_in_other, fc1_other)
        hidden, slope = gelu_parts(pre_act + fc1_bias.astype(jnp.float32))
        hidden_b = hidden.astype(jnp.bfloat16)

        def act_block(k):
            head_block = lax.dynamic_slice_in_dim(mixed_b, k * rows, rows, 1)
            ffn_block = lax.dynamic_slice_in_dim(hidden_b, k * fc2_rows, fc2_rows, 1)
            return jnp.concatenate([head_block, ffn_block], axis=1)

        acts_all = plane_rows(act_block)
        second_own = dot_first(acts_all, back_all).astype(jnp.bfloat16)
        fc2_mine, hidden_b, slope = lax.optimization_barrier((fc2_mine, hidden_b, slope))
        fc2_other = swap(fc2_mine)
        joined_all = plane_cols(d_joined)
        d_hidden = dot_last(back_cut_mine, fc2_mine) + dot_last(back_cut_other, fc2_other)
        d_pre = (d_hidden * slope).astype(jnp.bfloat16)
        pre_cut_mine = cut(d_pre, core, 1)
        pre_cut_other = swap(cut(d_pre, 1 - core, 1))
        piece_cols = pre_cut_mine.shape[1] // PRE_PIECES
        pre_all = []
        for piece in range(PRE_PIECES):
            span = slice(piece * piece_cols, (piece + 1) * piece_cols)
            pair = jnp.stack([pre_cut_mine[:, span], pre_cut_other[:, span]])
            pre_all.append(gathered(pair).reshape(-1, piece_cols))

        second_mine = line_sum(second_own, CHUNKS_A, place)
        second_other = swap(second_mine)
        qkv_grad_own = dot_first(normed_all, joined_all).astype(jnp.bfloat16)
        qkv_grad_mine = line_sum(qkv_grad_own, CHUNKS_B, place)
        qkv_grad_other = swap(qkv_grad_mine)
        fc1_mine_parts, fc1_other_parts = [], []
        for piece in range(PRE_PIECES):
            piece_own = dot_first(normed_all, pre_all[piece]).astype(jnp.bfloat16)
            piece_mine = line_sum(piece_own, CHUNKS_C, place)
            fc1_mine_parts.append(piece_mine)
            fc1_other_parts.append(swap(piece_mine))

        out_mine = dot_plain(mixed_b, dense_mine) + dot_plain(hidden_b, fc2_mine)
        out_other = dot_plain(mixed_b, dense_other) + dot_plain(hidden_b, fc2_other)
        layer_out = (
            token_rows
            + joined_halves(out_mine, out_other)
            + dense_bias.astype(jnp.float32)
            + fc2_bias.astype(jnp.float32)
        ).astype(jnp.bfloat16)
        d_normed = row_cols_back(
            dot_last(d_joined, qkv_mine) + dot_last(d_pre, fc1_mine),
            dot_last(d_joined, qkv_other) + dot_last(d_pre, fc1_other),
        )
        gain_sum = jnp.sum(d_normed * x_hat, axis=0)
        shift_sum = jnp.sum(d_normed, axis=0)
        d_hat = d_normed * gain_f32
        d_input = inv_std * (
            d_hat
            - jnp.mean(d_hat, axis=-1, keepdims=True)
            - x_hat * jnp.mean(d_hat * x_hat, axis=-1, keepdims=True)
        )
        back_f32 = back_b.astype(jnp.float32)
        input_grad = (back_f32 + d_input).astype(jnp.bfloat16)

        small = [
            gain_sum,
            shift_sum,
            jnp.sum(d_joined, axis=0, dtype=jnp.float32),
            jnp.sum(back_f32, axis=0),
            jnp.sum(d_pre, axis=0, dtype=jnp.float32),
        ]
        small_total = total_of(jnp.concatenate(small))
        owned, start = [], 0
        for piece in small:
            count = piece.shape[0] // groups
            owned.append(lax.dynamic_slice_in_dim(small_total, start + group * count, count, 0))
            start += piece.shape[0]

        core_index = core.reshape((1,)).astype(jnp.int32)
        return (
            layer_out.reshape(inputs.shape),
            input_grad.reshape(inputs.shape),
            owned[0],
            owned[1],
            assemble(core_index, [qkv_grad_mine], [qkv_grad_other], 0, rows),
            owned[2],
            assemble(core_index, [second_mine], [second_other], 0, rows),
            owned[3],
            assemble(core_index, fc1_mine_parts, fc1_other_parts, 0, rows),
            owned[4],
            assemble(core_index, [second_mine], [second_other], rows, fc2_rows),
            owned[3],
        )

    return per_device


def solution(mesh):
    placed = (
        P(AXES, None, None),
        P(AXES, None),
        P(AXES, None, None),
        P(),
        P(),
        P("fsdp", None),
        P(),
        P("fsdp", None),
        P(),
        P("fsdp", None),
        P(),
        P("fsdp", None),
        P(),
    )
    return jax.shard_map(
        make_per_device(mesh.shape["fsdp"], mesh.shape["rep"]),
        mesh=mesh,
        in_specs=placed,
        out_specs=(
            P(AXES, None, None),
            P(AXES, None, None),
            P("fsdp"),
            P("fsdp"),
            P("fsdp", None),
            P("fsdp"),
            P("fsdp", None),
            P("fsdp"),
            P("fsdp", None),
            P("fsdp"),
            P("fsdp", None),
            P("fsdp"),
        ),
        check_vma=False,
    )
```
